128 devices in a mesh: shard: 128 (over z, y, x, core).
Axes of the slice: x: 4, y: 4, z: 4, core: 2. Of those that a mesh axis runs over, the one named last changes fastest.
Arguments:
- picked_rows: int32 [4096, 8], P('shard'), may hold values from 0 to 65535
- main_table: float32 [65536, 128], P('shard'), may hold values from -6 to 6
- dense_part: float32 [4096, 128], P('shard'), may hold values from -6 to 6
- small_ids: int32 [4096], P('shard'), may hold values from 0 to 511
- small_table: float32 [512, 128], P('shard'), may hold values from -6 to 6
- scale_ids: int32 [4096], P('shard'), may hold values from 0 to 511
Outputs:
- features: float32 [4096, 3, 128], P('shard')
The draws below stay inside these ranges and needn't reach their ends.
All inputs are finite; a program needn't handle non-finite values.
Results may differ from the reference program's by a relative error of at most 0.0003.
Values sent between devices are 32-bit elements.
A program may use at most 64 MiB of HBM per device.

```python
import math
import jax
import jax.numpy as jnp
import numpy as np

EXAMPLES = 4096
FEATURES = 128
PICKS = 8
BIG_ROWS = 65536
SMALL_ROWS = 512


def place_ends(array, key, low, top_value):
    index_at = [jax.random.randint(jax.random.fold_in(key, axis), (), 0, length) for axis, length in enumerate(array.shape)]
    main_axis = array.shape.index(max(array.shape))
    beside = index_at[:main_axis] + [(index_at[main_axis] + 1) % array.shape[main_axis]] + index_at[main_axis + 1:]
    return array.at[tuple(index_at)].set(low).at[tuple(beside)].set(top_value)


def levels(key, dims, shards, least, top_value):
    gain, own = 1.0, jax.random.fold_in(key, 6)
    for position, shards_of in shards:
        steps = jnp.exp(jax.random.uniform(jax.random.fold_in(own, position), (shards_of,), jnp.float32, least / len(shards), top_value / len(shards)))
        gain = gain * jnp.repeat(steps, dims[position] // shards_of).reshape([-1 if axis == position else 1 for axis in range(len(dims))])
    return gain


def rank_bounds(count, lean):
    portions = [(1 << 20) // math.isqrt(standing ** lean) + 1 for standing in range(1, count + 1)]
    width = 1 + sum(portions) // (1 << 30)
    return np.cumsum(np.array([max(1, weight // width) for weight in portions]))


def skewed_ids(rng, extent, number_of, skew):
    listing = rank_bounds(number_of, skew)
    lot = jax.random.randint(jax.random.fold_in(rng, 1), extent, 0, int(listing[number_of - 1]))
    grade = jnp.searchsorted(jnp.asarray(listing, jnp.int32), lot, side="right")
    return jax.random.permutation(jax.random.fold_in(rng, 2), number_of)[grade].astype(jnp.int32)


def noise(rng, dims, scale, limit, cuts=(), dtype=jnp.bfloat16):
    values = scale * jax.random.normal(rng, dims, jnp.float32)
    if cuts:
        values = values * levels(rng, dims, cuts, -0.22, 0.18)
    return jnp.clip(values, -limit, limit).astype(dtype)


def setup_inputs(seed: int = 0) -> dict:
    key_of = jax.random.split(jax.random.key(seed), 7)
    return {
        "picked_rows": place_ends(skewed_ids(key_of[0], (EXAMPLES, PICKS), BIG_ROWS, 1), jax.random.fold_in(key_of[0], 3), 0, BIG_ROWS - 1).astype(jnp.int32),
        "main_table": noise(key_of[1], (BIG_ROWS, FEATURES), 1.0, 6.0, ((0, 128),), jnp.float32),
        "dense_part": noise(key_of[2], (EXAMPLES, FEATURES), 1.0, 6.0, ((0, 128),), jnp.float32),
        "small_ids": place_ends(jax.random.randint(key_of[3], (EXAMPLES,), 0, SMALL_ROWS), jax.random.fold_in(key_of[3], 1), 0, SMALL_ROWS - 1).astype(jnp.int32),
        "small_table": noise(key_of[4], (SMALL_ROWS, FEATURES), 1.0, 6.0, ((0, 128),), jnp.float32),
        "scale_ids": place_ends(skewed_ids(key_of[5], (EXAMPLES,), SMALL_ROWS, 1), jax.random.fold_in(key_of[5], 3), 0, SMALL_ROWS - 1).astype(jnp.int32),
    }


def reference(picked_rows, main_table, dense_part, small_ids, small_table, scale_ids):
    pooled = jnp.sum(main_table[picked_rows].astype(jnp.float32), axis=1) * PICKS ** -0.5
    small_rows = small_table[small_ids].astype(jnp.float32)
    dense_part = dense_part * small_table[scale_ids].astype(jnp.float32)
    features = jnp.stack([dense_part * pooled, pooled * small_rows, dense_part * small_rows], axis=1)
    return features
```

```python
import functools

import jax
import jax.numpy as jnp
from jax import lax
from jax.experimental import pallas as pl
from jax.experimental.pallas import tpu as pltpu
from jax.sharding import Mesh
from jax.sharding import PartitionSpec as P

PICKS = 8
SHARD = ("z", "y", "x", "c")
MESH = pl.DeviceIdType.MESH


def kernel(
    picks_hbm, table_hbm, dense_hbm, small_hbm, small_ids, scale_ids,
    out_ref,
    picks_in, ids, ids_t, count, table, split, total, part, got, small, dense, lhs_rows, scale_rows,
    load_sem, ids_send, ids_recv, tab_send, tab_recv, core_send, core_recv,
    small_send, small_recv, sum_send, sum_recv,
):
    z, y, x, c = (lax.axis_index(a) for a in SHARD)
    zy = z * 4 + y

    def peer(dz=0, dy=0, dx=0, dc=0):
        return (
            lax.rem(z + dz, 4), lax.rem(y + dy, 4), lax.rem(x + dx, 4), lax.rem(c + dc, 2)
        )

    def at_x(s):
        return lax.rem(x + 4 - s, 4)

    def send(src, dst, send_sem, recv_sem, to):
        copy = pltpu.make_async_remote_copy(
            src_ref=src, dst_ref=dst, send_sem=send_sem, recv_sem=recv_sem,
            device_id=to, device_id_type=MESH,
        )
        copy.start()
        return copy

    half = 256
    load_picks = pltpu.make_async_copy(picks_hbm, picks_in, load_sem.at[0])
    load_table = pltpu.make_async_copy(table_hbm, table.at[x, c], load_sem.at[1])
    load_small = pltpu.make_async_copy(small_hbm, small.at[c, x, zy], load_sem.at[2])
    load_dense = pltpu.make_async_copy(dense_hbm, dense, load_sem.at[3])
    load_table.start()
    load_picks.start()
    load_small.start()
    load_dense.start()

    axis_peers = (
        [peer(dx=d) for d in (1, 2, 3)] + [peer(dc=1)]
        + [peer(dy=d) for d in (1, 2, 3)] + [peer(dz=d) for d in (1, 2, 3)]
    )
    barrier = pltpu.get_barrier_semaphore()
    for who in axis_peers:
        pl.semaphore_signal(barrier, inc=1, device_id=who, device_id_type=MESH)
    pl.semaphore_wait(barrier, len(axis_peers))

    started = []

    def table_piece(s, h, core):
        return table.at[at_x(s), core, pl.ds(h * half, half)]

    def ring(s, h, step):
        piece = table_piece(s, h, c)
        k = ((s * 2 + h) * 2) + (0 if step == 1 else 1)
        copy = send(piece, piece, tab_send.at[k], tab_recv.at[k], peer(dx=step % 4))
        started.append(copy)
        return copy

    def arrived(k, piece, sem):
        pltpu.make_async_copy(piece, piece, sem.at[k]).wait()

    def cross(k, piece):
        started.append(send(piece, piece, core_send.at[k], core_recv.at[k], peer(dc=1)))

    load_table.wait()
    ring(0, 0, 1)
    ring(0, 1, -1)
    ring(0, 1, 1)
    ring(0, 0, -1)
    cross(0, table.at[x, c])

    load_picks.wait()
    ids[zy] = picks_in[...]
    load_small.wait()
    for d in (1, 2, 3):
        started.append(send(ids.at[zy], ids.at[zy], ids_send.at[d], ids_recv.at[d], peer(dy=d)))
        started.append(send(
            small.at[c, x, zy], small.at[c, x, zy], small_send.at[d], small_recv.at[d], peer(dy=d)
        ))
    for d in (1, 2, 3):
        came = z * 4 + lax.rem(y + 4 - d, 4)
        arrived(d, ids.at[came], ids_recv)
        arrived(d, small.at[c, x, came], small_recv)
    mine = pl.ds(z * 4, 4)
    for d in (1, 2, 3):
        started.append(send(
            ids.at[mine], ids.at[mine], ids_send.at[3 + d], ids_recv.at[3 + d], peer(dz=d)
        ))
        started.append(send(
            small.at[c, x, mine], small.at[c, x, mine],
            small_send.at[3 + d], small_recv.at[3 + d], peer(dz=d),
        ))

    def recv_index(s, h, step):
        return ((s * 2 + h) * 2) + (0 if step == 1 else 1)

    arrived(recv_index(0, 0, 1), table_piece(1, 0, c), tab_recv)
    ring(1, 0, 1)
    arrived(recv_index(0, 1, -1), table_piece(3, 1, c), tab_recv)
    ring(3, 1, -1)
    cross(1, table_piece(1, 0, c))
    cross(2, table_piece(3, 1, c))

    for d in (1, 2, 3):
        came = pl.ds(lax.rem(z + 4 - d, 4) * 4, 4)
        arrived(3 + d, ids.at[came], ids_recv)
        arrived(3 + d, small.at[c, x, came], small_recv)
    for d in (1, 2, 3):
        started.append(send(
            small.at[c, x], small.at[c, x], small_send.at[6 + d], small_recv.at[6 + d], peer(dx=d)
        ))

    first = zy * 4096
    for b in range(16):
        block = ids[b] - first
        block = jnp.concatenate([block, jnp.zeros((8, 96), jnp.int32)], axis=1)
        ids_t[b * 32 : (b + 1) * 32, :] = jnp.concatenate(
            [jnp.transpose(block)[:32], jnp.zeros((32, 120), jnp.int32)], axis=1
        )

    lane = lax.broadcasted_iota(jnp.int32, (8, 128), 1)

    def count_rows(s):
        base = at_x(s) * 1024

        def tile(t, carry):
            halves = []
            for u in range(2):
                rows = ids_t[pl.ds(pl.multiple_of(t * 16 + u * 8, 8), 8), :] - base
                halves.append([
                    jnp.broadcast_to(rows[:, k : k + 1], (8, 128)) for k in range(PICKS)
                ])
            for q in range(8):
                sums = []
                for u in range(2):
                    acc = None
                    for k in range(PICKS):
                        hit = jnp.where(halves[u][k] == lane + q * 128, 1.0, 0.0)
                        acc = hit if acc is None else acc + hit
                    sums.append(acc)
                count[s, pl.ds(pl.multiple_of(t * 16, 16), 16), q * 128 : (q + 1) * 128] = (
                    jnp.concatenate(sums, axis=0).astype(jnp.bfloat16)
                )
            return carry

        lax.fori_loop(0, 32, tile, 0)

    def add_product(s, start):
        for core in range(2):
            def cut(t, carry):
                at = pl.ds(pl.multiple_of(t * 64, 64), 64)
                rows = table[at_x(s), core, at]
                high = rows.astype(jnp.bfloat16)
                low = (rows - high.astype(jnp.float32)).astype(jnp.bfloat16)
                split[core, at, 0:128] = high
                split[core, at, 128:256] = low
                return carry

            lax.fori_loop(0, 8, cut, 0)

        def tile(t, carry):
            at = pl.ds(pl.multiple_of(t * 128, 128), 128)
            new = jnp.dot(
                count[s, at, :], split[...].reshape(1024, 256), preferred_element_type=jnp.float32
            )
            if start:
                total[at, :] = new
            else:
                total[at, :] = total[at, :] + new
            return carry

        lax.fori_loop(0, 4, tile, 0)

    count_rows(0)
    arrived(recv_index(0, 1, 1), table_piece(1, 1, c), tab_recv)
    cross(3, table_piece(1, 1, c))
    arrived(recv_index(0, 0, -1), table_piece(3, 0, c), tab_recv)
    cross(4, table_piece(3, 0, c))
    for d in (1, 2, 3):
        arrived(6 + d, small.at[c, at_x(d)], small_recv)
    started.append(send(small.at[c], small.at[c], small_send.at[10], small_recv.at[10], peer(dc=1)))
    count_rows(1)
    count_rows(2)
    arrived(recv_index(1, 0, 1), table_piece(2, 0, c), tab_recv)
    cross(5, table_piece(2, 0, c))
    arrived(recv_index(3, 1, -1), table_piece(2, 1, c), tab_recv)
    cross(6, table_piece(2, 1, c))
    count_rows(3)

    o = 1 - c
    arrived(0, table.at[x, o], core_recv)
    add_product(0, True)
    arrived(1, table_piece(1, 0, o), core_recv)
    arrived(3, table_piece(1, 1, o), core_recv)
    add_product(1, False)
    arrived(2, table_piece(3, 1, o), core_recv)
    arrived(4, table_piece(3, 0, o), core_recv)
    add_product(3, False)
    arrived(5, table_piece(2, 0, o), core_recv)
    arrived(6, table_piece(2, 1, o), core_recv)
    add_product(2, False)
    part[...] = (total[:, :128] + total[:, 128:]).reshape(16, 32, 128)

    for j in range(1, 16):
        dz, dy = divmod(j, 4)
        to = peer(dz=dz, dy=dy)
        started.append(send(
            part.at[to[0] * 4 + to[1]], got.at[j], sum_send.at[j], sum_recv.at[j], to
        ))

    arrived(10, small.at[o], small_recv)
    load_dense.wait()

    def small_row(i):
        core, place = lax.rem(lax.div(i, 4), 2), lax.rem(lax.div(i, 8), 4)
        return small[core, place, lax.div(i, 32), pl.ds(lax.rem(i, 4), 1), :]

    for e in range(32):
        lhs_rows[e : e + 1, :] = small_row(small_ids[e])
        scale_rows[e : e + 1, :] = small_row(scale_ids[e])
    rows = lhs_rows[...]
    scaled = dense[...] * scale_rows[...]
    out_ref[2] = scaled * rows

    pooled = part[zy]
    for j in range(1, 16):
        arrived(j, got.at[j], sum_recv)
        pooled = pooled + got[j]
    pooled = pooled * PICKS ** (-0.5)
    out_ref[0] = scaled * pooled
    out_ref[1] = pooled * rows
    for copy in started:
        copy.wait_send()


def on_device(picked_rows, main_table, dense_part, small_ids, small_table, scale_ids):
    dma = pltpu.SemaphoreType.DMA
    f32 = jnp.float32
    out = pl.pallas_call(
        kernel,
        out_shape=jax.ShapeDtypeStruct((3, 32, 128), f32),
        in_specs=[pl.BlockSpec(memory_space=pl.ANY)] * 4
        + [pl.BlockSpec(memory_space=pltpu.SMEM)] * 2,
        out_specs=pl.BlockSpec(memory_space=pltpu.VMEM),
        scratch_shapes=[
            pltpu.VMEM((8, 32), jnp.int32),
            pltpu.VMEM((16, 8, 32), jnp.int32),
            pltpu.VMEM((512, 128), jnp.int32),
            pltpu.VMEM((4, 512, 1024), jnp.bfloat16),
            pltpu.VMEM((4, 2, 512, 128), f32),
            pltpu.VMEM((2, 512, 256), jnp.bfloat16),
            pltpu.VMEM((512, 256), f32),
            pltpu.VMEM((16, 32, 128), f32),
            pltpu.VMEM((16, 32, 128), f32),
            pltpu.VMEM((2, 4, 16, 4, 128), f32),
            pltpu.VMEM((32, 128), f32),
            pltpu.VMEM((32, 128), f32),
            pltpu.VMEM((32, 128), f32),
            dma((4,)), dma((7,)), dma((7,)), dma((16,)), dma((16,)), dma((7,)), dma((7,)),
            dma((11,)), dma((11,)), dma((16,)), dma((16,)),
        ],
        compiler_params=pltpu.CompilerParams(collective_id=0, has_side_effects=True),
    )(picked_rows.T, main_table, dense_part, small_table, small_ids, scale_ids)
    return out.transpose(1, 0, 2)


def solution(mesh):
    split = Mesh(mesh.devices.reshape(4, 4, 4, 2), SHARD)
    placed = (P(SHARD, None), P(SHARD, None), P(SHARD, None), P(SHARD), P(SHARD, None), P(SHARD))
    return jax.shard_map(
        on_device, mesh=split, in_specs=placed, out_specs=P(SHARD, None, None), check_vma=False
    )
```

```python
import functools

import jax
import jax.numpy as jnp
from jax import lax
from jax.experimental import pallas as pl
from jax.experimental.pallas import tpu as pltpu
from jax.sharding import Mesh
from jax.sharding import PartitionSpec as P

PICKS = 8
SHARD = ("z", "y", "x", "c")
MESH = pl.DeviceIdType.MESH


def kernel(
    picks_hbm, table_hbm, dense_hbm, small_hbm, small_ids_hbm, scale_ids_hbm,
    out_ref,
    small_ids, scale_ids, picks_in, ids, spread, count, table, split, total, part, got, small, dense, lhs_rows, scale_rows,
    load_sem, ids_send, ids_recv, tab_send, tab_recv, core_send, core_recv,
    small_send, small_recv, sum_send, sum_recv,
):
    z, y, x, c = (lax.axis_index(a) for a in SHARD)
    zy = z * 4 + y

    def peer(dz=0, dy=0, dx=0, dc=0):
        return (
            lax.rem(z + dz, 4), lax.rem(y + dy, 4), lax.rem(x + dx, 4), lax.rem(c + dc, 2)
        )

    def at_x(s):
        return lax.rem(x + 4 - s, 4)

    def send(src, dst, send_sem, recv_sem, to):
        copy = pltpu.make_async_remote_copy(
            src_ref=src, dst_ref=dst, send_sem=send_sem, recv_sem=recv_sem,
            device_id=to, device_id_type=MESH,
        )
        copy.start()
        return copy

    half = 256
    load_picks = pltpu.make_async_copy(picks_hbm, picks_in, load_sem.at[0])
    load_table = pltpu.make_async_copy(table_hbm, table.at[x, c], load_sem.at[1])
    load_small = pltpu.make_async_copy(small_hbm, small.at[c, x, zy], load_sem.at[2])
    load_dense = pltpu.make_async_copy(dense_hbm, dense, load_sem.at[3])
    load_table.start()
    load_picks.start()
    load_small.start()
    load_dense.start()
    load_ids = [
        pltpu.make_async_copy(small_ids_hbm, small_ids, load_sem.at[4]),
        pltpu.make_async_copy(scale_ids_hbm, scale_ids, load_sem.at[5]),
    ]
    for load in load_ids:
        load.start()

    axis_peers = (
        [peer(dx=d) for d in (1, 2, 3)] + [peer(dc=1)]
        + [peer(dy=d) for d in (1, 2, 3)] + [peer(dz=d) for d in (1, 2, 3)]
    )
    barrier = pltpu.get_barrier_semaphore()
    for who in axis_peers:
        pl.semaphore_signal(barrier, inc=1, device_id=who, device_id_type=MESH)
    pl.semaphore_wait(barrier, len(axis_peers))

    started = []

    def table_piece(s, h, core):
        return table.at[at_x(s), core, pl.ds(h * half, half)]

    def ring(s, h, step):
        piece = table_piece(s, h, c)
        k = ((s * 2 + h) * 2) + (0 if step == 1 else 1)
        copy = send(piece, piece, tab_send.at[k], tab_recv.at[k], peer(dx=step % 4))
        started.append(copy)
        return copy

    def arrived(k, piece, sem):
        pltpu.make_async_copy(piece, piece, sem.at[k]).wait()

    def cross(k, piece):
        started.append(send(piece, piece, core_send.at[k], core_recv.at[k], peer(dc=1)))

    load_table.wait()
    ring(0, 0, 1)
    ring(0, 1, -1)
    ring(0, 1, 1)
    ring(0, 0, -1)
    cross(0, table.at[x, c])

    load_picks.wait()
    ids[zy] = picks_in[...]
    load_small.wait()
    for d in (1, 2, 3):
        started.append(send(ids.at[zy], ids.at[zy], ids_send.at[d], ids_recv.at[d], peer(dy=d)))
        started.append(send(
            small.at[c, x, zy], small.at[c, x, zy], small_send.at[d], small_recv.at[d], peer(dy=d)
        ))
    for d in (1, 2, 3):
        came = z * 4 + lax.rem(y + 4 - d, 4)
        arrived(d, ids.at[came], ids_recv)
        arrived(d, small.at[c, x, came], small_recv)
    mine = pl.ds(z * 4, 4)
    for d in (1, 2, 3):
        started.append(send(
            ids.at[mine], ids.at[mine], ids_send.at[3 + d], ids_recv.at[3 + d], peer(dz=d)
        ))
        started.append(send(
            small.at[c, x, mine], small.at[c, x, mine],
            small_send.at[3 + d], small_recv.at[3 + d], peer(dz=d),
        ))

    def recv_index(s, h, step):
        return ((s * 2 + h) * 2) + (0 if step == 1 else 1)

    arrived(recv_index(0, 0, 1), table_piece(1, 0, c), tab_recv)
    ring(1, 0, 1)
    arrived(recv_index(0, 1, -1), table_piece(3, 1, c), tab_recv)
    ring(3, 1, -1)
    cross(1, table_piece(1, 0, c))
    cross(2, table_piece(3, 1, c))

    for d in (1, 2, 3):
        came = pl.ds(lax.rem(z + 4 - d, 4) * 4, 4)
        arrived(3 + d, ids.at[came], ids_recv)
        arrived(3 + d, small.at[c, x, came], small_recv)
    for d in (1, 2, 3):
        started.append(send(
            small.at[c, x], small.at[c, x], small_send.at[6 + d], small_recv.at[6 + d], peer(dx=d)
        ))

    first = zy * 4096
    for b in range(16):
        block = jnp.clip(ids[b] - first, -1, 4096)
        block = jnp.concatenate([block, jnp.zeros((8, 96), jnp.int32)], axis=1)
        columns = jnp.transpose(block)[:32]
        for k in range(PICKS):
            spread[k, b * 32 : (b + 1) * 32, :] = jnp.broadcast_to(
                columns[:, k : k + 1], (32, 128)
            ).astype(jnp.int16)
    one, none = jnp.ones((16, 128), jnp.bfloat16), jnp.zeros((16, 128), jnp.bfloat16)
    lane = lax.broadcasted_iota(jnp.int32, (16, 128), 1).astype(jnp.int16)

    def count_rows(places):
        def tile(t, carry):
            at = pl.ds(pl.multiple_of(t * 16, 16), 16)
            wanted = [spread[k, at, :] for k in range(PICKS)]
            for place in places:
                for q in range(8):
                    here = lane + jnp.int16(place * 1024 + q * 128)
                    hits = [jnp.where(w == here, one, none) for w in wanted]
                    while len(hits) > 1:
                        hits = [a + b for a, b in zip(hits[::2], hits[1::2])]
                    count[place, at, q * 128 : (q + 1) * 128] = hits[0]
            return carry

        lax.fori_loop(0, 32, tile, 0)

    def cut_rows(s, core):
        def cut(t, carry):
            at = pl.ds(pl.multiple_of(t * 128, 128), 128)
            rows = table[at_x(s), core, at]
            high = rows.astype(jnp.bfloat16)
            low = (rows - high.astype(jnp.float32)).astype(jnp.bfloat16)
            split[s, core, at, 0:128] = high
            split[s, core, at, 128:256] = low
            return carry

        lax.fori_loop(0, 4, cut, 0)

    def add_product(s, start):
        new = jnp.dot(
            count[at_x(s)], split[s].reshape(1024, 256), preferred_element_type=jnp.float32
        )
        total[...] = new if start else total[...] + new

    count_rows((0, 1))
    arrived(recv_index(0, 1, 1), table_piece(1, 1, c), tab_recv)
    cross(3, table_piece(1, 1, c))
    arrived(recv_index(0, 0, -1), table_piece(3, 0, c), tab_recv)
    cross(4, table_piece(3, 0, c))
    for d in (1, 2, 3):
        arrived(6 + d, small.at[c, at_x(d)], small_recv)
    started.append(send(small.at[c], small.at[c], small_send.at[10], small_recv.at[10], peer(dc=1)))
    count_rows((2, 3))
    o = 1 - c
    cut_rows(0, c)
    arrived(0, table.at[x, o], core_recv)
    cut_rows(0, o)
    add_product(0, True)
    arrived(recv_index(1, 0, 1), table_piece(2, 0, c), tab_recv)
    cross(5, table_piece(2, 0, c))
    arrived(recv_index(3, 1, -1), table_piece(2, 1, c), tab_recv)
    cross(6, table_piece(2, 1, c))
    arrived(1, table_piece(1, 0, o), core_recv)
    arrived(3, table_piece(1, 1, o), core_recv)
    cut_rows(1, c)
    cut_rows(1, o)
    add_product(1, False)
    arrived(2, table_piece(3, 1, o), core_recv)
    arrived(4, table_piece(3, 0, o), core_recv)
    cut_rows(3, c)
    cut_rows(3, o)
    add_product(3, False)
    cut_rows(2, c)
    arrived(5, table_piece(2, 0, o), core_recv)
    arrived(6, table_piece(2, 1, o), core_recv)
    cut_rows(2, o)
    add_product(2, False)
    part[...] = (total[:, :128] + total[:, 128:]).reshape(16, 32, 128)

    for j in range(1, 16):
        dz, dy = divmod(j, 4)
        to = peer(dz=dz, dy=dy)
        started.append(send(
            part.at[to[0] * 4 + to[1]], got.at[j], sum_send.at[j], sum_recv.at[j], to
        ))

    arrived(10, small.at[o], small_recv)
    load_dense.wait()
    for load in load_ids:
        load.wait()

    def small_row(i):
        core, place = lax.rem(lax.div(i, 4), 2), lax.rem(lax.div(i, 8), 4)
        return small[core, place, lax.div(i, 32), pl.ds(lax.rem(i, 4), 1), :]

    for e in range(32):
        lhs_rows[e : e + 1, :] = small_row(small_ids[e])
        scale_rows[e : e + 1, :] = small_row(scale_ids[e])
    rows = lhs_rows[...]
    scaled = dense[...] * scale_rows[...]
    out_ref[2] = scaled * rows

    pooled = part[zy]
    for j in range(1, 16):
        arrived(j, got.at[j], sum_recv)
        pooled = pooled + got[j]
    pooled = pooled * PICKS ** (-0.5)
    out_ref[0] = scaled * pooled
    out_ref[1] = pooled * rows
    for copy in started:
        copy.wait_send()


def on_device(picked_rows, main_table, dense_part, small_ids, small_table, scale_ids):
    dma = pltpu.SemaphoreType.DMA
    f32 = jnp.float32
    out = pl.pallas_call(
        kernel,
        out_shape=pltpu.VMEM((3, 32, 128), f32),
        in_specs=[pl.BlockSpec(memory_space=pl.ANY)] * 6,
        out_specs=pl.BlockSpec(memory_space=pltpu.VMEM),
        scratch_shapes=[
            pltpu.SMEM((32,), jnp.int32),
            pltpu.SMEM((32,), jnp.int32),
            pltpu.VMEM((8, 32), jnp.int32),
            pltpu.VMEM((16, 8, 32), jnp.int32),
            pltpu.VMEM((8, 512, 128), jnp.int16),
            pltpu.VMEM((4, 512, 1024), jnp.bfloat16),
            pltpu.VMEM((4, 2, 512, 128), f32),
            pltpu.VMEM((4, 2, 512, 256), jnp.bfloat16),
            pltpu.VMEM((512, 256), f32),
            pltpu.VMEM((16, 32, 128), f32),
            pltpu.VMEM((16, 32, 128), f32),
            pltpu.VMEM((2, 4, 16, 4, 128), f32),
            pltpu.VMEM((32, 128), f32),
            pltpu.VMEM((32, 128), f32),
            pltpu.VMEM((32, 128), f32),
            dma((6,)), dma((7,)), dma((7,)), dma((16,)), dma((16,)), dma((7,)), dma((7,)),
            dma((11,)), dma((11,)), dma((16,)), dma((16,)),
        ],
        compiler_params=pltpu.CompilerParams(collective_id=0, has_side_effects=True),
    )(picked_rows.T, main_table, dense_part, small_table, small_ids, scale_ids)
    return out.transpose(1, 0, 2)


def solution(mesh):
    split = Mesh(mesh.devices.reshape(4, 4, 4, 2), SHARD)
    placed = (P(SHARD, None), P(SHARD, None), P(SHARD, None), P(SHARD), P(SHARD, None), P(SHARD))
    return jax.shard_map(
        on_device, mesh=split, in_specs=placed, out_specs=P(SHARD, None, None), check_vma=False
    )
```

```python
import functools

import jax
import jax.numpy as jnp
from jax import lax
from jax.experimental import pallas as pl
from jax.experimental.pallas import tpu as pltpu
from jax.sharding import Mesh
from jax.sharding import PartitionSpec as P

PICKS = 8
SHARD = ("z", "y", "x", "c")
MESH = pl.DeviceIdType.MESH


def kernel(
    picks_hbm, table_hbm, dense_hbm, small_hbm, small_ids_hbm, scale_ids_hbm,
    out_ref,
    small_ids, scale_ids, picks_in, ids, spread, count, table, split, total, part, got, small, dense, lhs_rows, scale_rows,
    load_sem, ids_send, ids_recv, tab_send, tab_recv, core_send, core_recv,
    small_send, small_recv, sum_send, sum_recv,
):
    z, y, x, c = (lax.axis_index(a) for a in SHARD)
    zy = z * 4 + y

    def peer(dz=0, dy=0, dx=0, dc=0):
        return (
            lax.rem(z + dz, 4), lax.rem(y + dy, 4), lax.rem(x + dx, 4), lax.rem(c + dc, 2)
        )

    def at_x(s):
        return lax.rem(x + 4 - s, 4)

    def send(src, dst, send_sem, recv_sem, to):
        copy = pltpu.make_async_remote_copy(
            src_ref=src, dst_ref=dst, send_sem=send_sem, recv_sem=recv_sem,
            device_id=to, device_id_type=MESH,
        )
        copy.start()
        return copy

    half = 256
    load_picks = pltpu.make_async_copy(picks_hbm, picks_in, load_sem.at[0])
    load_table = pltpu.make_async_copy(table_hbm, table.at[x, c], load_sem.at[1])
    load_small = pltpu.make_async_copy(small_hbm, small.at[c, x, zy], load_sem.at[2])
    load_dense = pltpu.make_async_copy(dense_hbm, dense, load_sem.at[3])
    load_table.start()
    load_picks.start()
    load_small.start()
    load_dense.start()
    load_ids = [
        pltpu.make_async_copy(small_ids_hbm, small_ids, load_sem.at[4]),
        pltpu.make_async_copy(scale_ids_hbm, scale_ids, load_sem.at[5]),
    ]
    for load in load_ids:
        load.start()

    axis_peers = (
        [peer(dx=d) for d in (1, 2, 3)] + [peer(dc=1)]
        + [peer(dy=d) for d in (1, 2, 3)] + [peer(dz=d) for d in (1, 2, 3)]
    )
    barrier = pltpu.get_barrier_semaphore()
    for who in axis_peers:
        pl.semaphore_signal(barrier, inc=1, device_id=who, device_id_type=MESH)
    pl.semaphore_wait(barrier, len(axis_peers))

    started = []

    def table_piece(s, h, core):
        return table.at[at_x(s), core, pl.ds(h * half, half)]

    def ring(s, h, step):
        piece = table_piece(s, h, c)
        k = ((s * 2 + h) * 2) + (0 if step == 1 else 1)
        copy = send(piece, piece, tab_send.at[k], tab_recv.at[k], peer(dx=step % 4))
        started.append(copy)
        return copy

    def arrived(k, piece, sem):
        pltpu.make_async_copy(piece, piece, sem.at[k]).wait()

    def cross(k, piece):
        started.append(send(piece, piece, core_send.at[k], core_recv.at[k], peer(dc=1)))

    load_table.wait()
    ring(0, 0, 1)
    ring(0, 1, -1)
    ring(0, 1, 1)
    ring(0, 0, -1)
    cross(0, table.at[x, c])

    load_picks.wait()
    ids[zy] = picks_in[...]
    load_small.wait()
    for d in (1, 2, 3):
        started.append(send(ids.at[zy], ids.at[zy], ids_send.at[d], ids_recv.at[d], peer(dy=d)))
        started.append(send(
            small.at[c, x, zy], small.at[c, x, zy], small_send.at[d], small_recv.at[d], peer(dy=d)
        ))
    for d in (1, 2, 3):
        came = z * 4 + lax.rem(y + 4 - d, 4)
        arrived(d, ids.at[came], ids_recv)
        arrived(d, small.at[c, x, came], small_recv)
    mine = pl.ds(z * 4, 4)
    for d in (1, 2, 3):
        started.append(send(
            ids.at[mine], ids.at[mine], ids_send.at[3 + d], ids_recv.at[3 + d], peer(dz=d)
        ))
        started.append(send(
            small.at[c, x, mine], small.at[c, x, mine],
            small_send.at[3 + d], small_recv.at[3 + d], peer(dz=d),
        ))

    first = zy * 4096

    def spread_picks(plane):
        for b in range(4):
            block = jnp.clip(ids[plane * 4 + b] - first, -1, 4096)
            block = jnp.concatenate([block, jnp.zeros((8, 96), jnp.int32)], axis=1)
            columns = jnp.transpose(block)[:32]
            for k in range(PICKS):
                spread[k, plane, b * 32 : (b + 1) * 32, :] = jnp.broadcast_to(
                    columns[:, k : k + 1], (32, 256)
                ).astype(jnp.int16)

    one, none = jnp.ones((16, 256), jnp.bfloat16), jnp.zeros((16, 256), jnp.bfloat16)
    lane = lax.broadcasted_iota(jnp.int32, (16, 256), 1).astype(jnp.int16)

    def count_rows(plane):
        def tile(t, carry):
            at = pl.ds(pl.multiple_of(t * 16, 16), 16)
            wanted = [spread[k, plane, at, :] for k in range(PICKS)]
            for place in range(4):
                for q in range(4):
                    here = lane + jnp.int16(place * 1024 + q * 256)
                    hits = [jnp.where(w == here, one, none) for w in wanted]
                    while len(hits) > 1:
                        hits = [a + b for a, b in zip(hits[::2], hits[1::2])]
                    count[place, plane, at, q * 256 : (q + 1) * 256] = hits[0]
            return carry

        lax.fori_loop(0, 8, tile, 0)

    def cut_rows(s, core):
        def cut(t, carry):
            at = pl.ds(pl.multiple_of(t * 128, 128), 128)
            rows = table[at_x(s), core, at]
            high = rows.astype(jnp.bfloat16)
            low = (rows - high.astype(jnp.float32)).astype(jnp.bfloat16)
            split[s, core, at, 0:128] = high
            split[s, core, at, 128:256] = low
            return carry

        lax.fori_loop(0, 4, cut, 0)

    def add_product(s, start):
        new = jnp.dot(
            count[at_x(s)].reshape(512, 1024), split[s].reshape(1024, 256), preferred_element_type=jnp.float32
        )
        total[...] = new if start else total[...] + new

    def recv_index(s, h, step):
        return ((s * 2 + h) * 2) + (0 if step == 1 else 1)

    spread_picks(z)
    count_rows(z)
    o = 1 - c
    cut_rows(0, c)
    arrived(recv_index(0, 0, 1), table_piece(1, 0, c), tab_recv)
    ring(1, 0, 1)
    arrived(recv_index(0, 1, -1), table_piece(3, 1, c), tab_recv)
    ring(3, 1, -1)
    cross(1, table_piece(1, 0, c))
    cross(2, table_piece(3, 1, c))

    for d in (1, 2, 3):
        came = lax.rem(z + 4 - d, 4)
        arrived(3 + d, ids.at[pl.ds(came * 4, 4)], ids_recv)
        spread_picks(came)
        count_rows(came)
    arrived(recv_index(0, 1, 1), table_piece(1, 1, c), tab_recv)
    cross(3, table_piece(1, 1, c))
    arrived(recv_index(0, 0, -1), table_piece(3, 0, c), tab_recv)
    cross(4, table_piece(3, 0, c))
    for d in (1, 2, 3):
        arrived(3 + d, small.at[c, x, pl.ds(lax.rem(z + 4 - d, 4) * 4, 4)], small_recv)
    for d in (1, 2, 3):
        started.append(send(
            small.at[c, x], small.at[c, x], small_send.at[6 + d], small_recv.at[6 + d], peer(dx=d)
        ))
    arrived(0, table.at[x, o], core_recv)
    cut_rows(0, o)
    add_product(0, True)
    arrived(recv_index(1, 0, 1), table_piece(2, 0, c), tab_recv)
    cross(5, table_piece(2, 0, c))
    arrived(recv_index(3, 1, -1), table_piece(2, 1, c), tab_recv)
    cross(6, table_piece(2, 1, c))
    arrived(1, table_piece(1, 0, o), core_recv)
    arrived(3, table_piece(1, 1, o), core_recv)
    cut_rows(1, c)
    cut_rows(1, o)
    add_product(1, False)
    arrived(2, table_piece(3, 1, o), core_recv)
    arrived(4, table_piece(3, 0, o), core_recv)
    cut_rows(3, c)
    cut_rows(3, o)
    add_product(3, False)
    cut_rows(2, c)
    arrived(5, table_piece(2, 0, o), core_recv)
    arrived(6, table_piece(2, 1, o), core_recv)
    cut_rows(2, o)
    add_product(2, False)
    part[...] = (total[:, :128] + total[:, 128:]).reshape(16, 32, 128)

    for j in range(1, 16):
        dz, dy = divmod(j, 4)
        to = peer(dz=dz, dy=dy)
        started.append(send(
            part.at[to[0] * 4 + to[1]], got.at[j], sum_send.at[j], sum_recv.at[j], to
        ))

    for d in (1, 2, 3):
        arrived(6 + d, small.at[c, at_x(d)], small_recv)
    started.append(send(small.at[c], small.at[c], small_send.at[10], small_recv.at[10], peer(dc=1)))
    arrived(10, small.at[o], small_recv)
    load_dense.wait()
    for load in load_ids:
        load.wait()

    def small_row(i):
        core, place = lax.rem(lax.div(i, 4), 2), lax.rem(lax.div(i, 8), 4)
        return small[core, place, lax.div(i, 32), pl.ds(lax.rem(i, 4), 1), :]

    for e in range(32):
        lhs_rows[e : e + 1, :] = small_row(small_ids[e])
        scale_rows[e : e + 1, :] = small_row(scale_ids[e])
    rows = lhs_rows[...]
    scaled = dense[...] * scale_rows[...]
    out_ref[2] = scaled * rows

    pooled = part[zy]
    for j in range(1, 16):
        arrived(j, got.at[j], sum_recv)
        pooled = pooled + got[j]
    pooled = pooled * PICKS ** (-0.5)
    out_ref[0] = scaled * pooled
    out_ref[1] = pooled * rows
    for copy in started:
        copy.wait_send()


def on_device(picked_rows, main_table, dense_part, small_ids, small_table, scale_ids):
    dma = pltpu.SemaphoreType.DMA
    f32 = jnp.float32
    out = pl.pallas_call(
        kernel,
        out_shape=pltpu.VMEM((3, 32, 128), f32),
        in_specs=[pl.BlockSpec(memory_space=pl.ANY)] * 6,
        out_specs=pl.BlockSpec(memory_space=pltpu.VMEM),
        scratch_shapes=[
            pltpu.SMEM((32,), jnp.int32),
            pltpu.SMEM((32,), jnp.int32),
            pltpu.VMEM((8, 32), jnp.int32),
            pltpu.VMEM((16, 8, 32), jnp.int32),
            pltpu.VMEM((8, 4, 128, 256), jnp.int16),
            pltpu.VMEM((4, 4, 128, 1024), jnp.bfloat16),
            pltpu.VMEM((4, 2, 512, 128), f32),
            pltpu.VMEM((4, 2, 512, 256), jnp.bfloat16),
            pltpu.VMEM((512, 256), f32),
            pltpu.VMEM((16, 32, 128), f32),
            pltpu.VMEM((16, 32, 128), f32),
            pltpu.VMEM((2, 4, 16, 4, 128), f32),
            pltpu.VMEM((32, 128), f32),
            pltpu.VMEM((32, 128), f32),
            pltpu.VMEM((32, 128), f32),
            dma((6,)), dma((7,)), dma((7,)), dma((16,)), dma((16,)), dma((7,)), dma((7,)),
            dma((11,)), dma((11,)), dma((16,)), dma((16,)),
        ],
        compiler_params=pltpu.CompilerParams(collective_id=0, has_side_effects=True),
    )(picked_rows.T, main_table, dense_part, small_table, small_ids, scale_ids)
    return out.transpose(1, 0, 2)


def solution(mesh):
    split = Mesh(mesh.devices.reshape(4, 4, 4, 2), SHARD)
    placed = (P(SHARD, None), P(SHARD, None), P(SHARD, None), P(SHARD), P(SHARD, None), P(SHARD))
    return jax.shard_map(
        on_device, mesh=split, in_specs=placed, out_specs=P(SHARD, None, None), check_vma=False
    )
```

```python
import functools

import jax
import jax.numpy as jnp
from jax import lax
from jax.experimental import pallas as pl
from jax.experimental.pallas import tpu as pltpu
from jax.sharding import Mesh
from jax.sharding import PartitionSpec as P

PICKS = 8
SHARD = ("z", "y", "x", "c")
MESH = pl.DeviceIdType.MESH


def kernel(
    picks_hbm, table_hbm, dense_hbm, small_hbm, small_ids_hbm, scale_ids_hbm,
    out_ref,
    small_ids, scale_ids, picks_in, ids, spread, count, table, split, total, part, got, small, dense, lhs_rows, scale_rows,
    load_sem, ids_send, ids_recv, tab_send, tab_recv, core_send, core_recv,
    small_send, small_recv, sum_send, sum_recv,
):
    z, y, x, c = (lax.axis_index(a) for a in SHARD)
    zy = z * 4 + y

    def peer(dz=0, dy=0, dx=0, dc=0):
        return (
            lax.rem(z + dz, 4), lax.rem(y + dy, 4), lax.rem(x + dx, 4), lax.rem(c + dc, 2)
        )

    def at_x(s):
        return lax.rem(x + 4 - s, 4)

    def send(src, dst, send_sem, recv_sem, to):
        copy = pltpu.make_async_remote_copy(
            src_ref=src, dst_ref=dst, send_sem=send_sem, recv_sem=recv_sem,
            device_id=to, device_id_type=MESH,
        )
        copy.start()
        return copy

    half = 256
    load_picks = pltpu.make_async_copy(picks_hbm, picks_in, load_sem.at[0])
    load_table = pltpu.make_async_copy(table_hbm, table.at[x, c], load_sem.at[1])
    load_small = pltpu.make_async_copy(small_hbm, small.at[c, x, zy], load_sem.at[2])
    load_dense = pltpu.make_async_copy(dense_hbm, dense, load_sem.at[3])
    load_table.start()
    load_picks.start()
    load_small.start()
    load_dense.start()
    load_ids = [
        pltpu.make_async_copy(small_ids_hbm, small_ids, load_sem.at[4]),
        pltpu.make_async_copy(scale_ids_hbm, scale_ids, load_sem.at[5]),
    ]
    for load in load_ids:
        load.start()

    axis_peers = (
        [peer(dx=d) for d in (1, 2, 3)] + [peer(dc=1)]
        + [peer(dy=d) for d in (1, 2, 3)] + [peer(dz=d) for d in (1, 2, 3)]
    )
    barrier = pltpu.get_barrier_semaphore()
    for who in axis_peers:
        pl.semaphore_signal(barrier, inc=1, device_id=who, device_id_type=MESH)
    pl.semaphore_wait(barrier, len(axis_peers))


    def table_piece(s, h, core):
        return table.at[at_x(s), core, pl.ds(h * half, half)]

    def ring(s, h, step, k):
        piece = table_piece(s, h, c)
        send(piece, piece, tab_send.at[0], tab_recv.at[k], peer(dx=step % 4))

    def arrived(k, piece, sem):
        pltpu.make_async_copy(piece, piece, sem.at[k]).wait()

    def cross(k, piece):
        send(piece, piece, core_send.at[0], core_recv.at[k], peer(dc=1))

    load_picks.wait()
    ids[zy] = picks_in[...]
    for d in (2, 1, 3):
        send(ids.at[zy], ids.at[zy], ids_send.at[0], ids_recv.at[0], peer(dy=d))
    load_table.wait()
    ring(0, 0, 1, 0)
    ring(0, 1, -1, 1)
    ring(0, 1, 1, 2)
    ring(0, 0, -1, 3)
    cross(0, table.at[x, c])
    load_small.wait()
    for d in (2, 1, 3):
        own = small.at[c, x, zy]
        send(own, own, small_send.at[0], small_recv.at[0], peer(dy=d))
    arrived(0, ids.at[pl.ds(0, 3)], ids_recv)
    mine = pl.ds(z * 4, 4)
    for d in (2, 1, 3):
        send(ids.at[mine], ids.at[mine], ids_send.at[1], ids_recv.at[d], peer(dz=d))
    arrived(0, small.at[0, 0, pl.ds(0, 3)], small_recv)
    for d in (1, 2, 3):
        own = small.at[c, x, mine]
        send(own, own, small_send.at[1], small_recv.at[1], peer(dz=d))

    first = zy * 4096

    def spread_picks(plane):
        for b in range(4):
            block = jnp.clip(ids[plane * 4 + b] - first, -1, 4096)
            block = jnp.concatenate([block, jnp.zeros((8, 96), jnp.int32)], axis=1)
            columns = jnp.transpose(block)[:32]
            for k in range(PICKS):
                spread[k, plane, b * 32 : (b + 1) * 32, :] = jnp.broadcast_to(
                    columns[:, k : k + 1], (32, 256)
                ).astype(jnp.int16)

    one, none = jnp.ones((16, 256), jnp.bfloat16), jnp.zeros((16, 256), jnp.bfloat16)
    lane = lax.broadcasted_iota(jnp.int32, (16, 256), 1).astype(jnp.int16)

    def count_rows(plane):
        def tile(t, carry):
            at = pl.ds(pl.multiple_of(t * 16, 16), 16)
            wanted = [spread[k, plane, at, :] for k in range(PICKS)]
            for place in range(4):
                for q in range(4):
                    here = lane + jnp.int16(place * 1024 + q * 256)
                    hits = [jnp.where(w == here, one, none) for w in wanted]
                    while len(hits) > 1:
                        hits = [a + b for a, b in zip(hits[::2], hits[1::2])]
                    count[place, plane, at, q * 256 : (q + 1) * 256] = hits[0]
            return carry

        lax.fori_loop(0, 8, tile, 0)

    def cut_rows(s, core):
        def cut(t, carry):
            at = pl.ds(pl.multiple_of(t * 128, 128), 128)
            rows = table[at_x(s), core, at]
            high = rows.astype(jnp.bfloat16)
            low = (rows - high.astype(jnp.float32)).astype(jnp.bfloat16)
            split[(0, 1, 3, 2)[s], core, at, 0:128] = high
            split[(0, 1, 3, 2)[s], core, at, 128:256] = low
            return carry

        lax.fori_loop(0, 4, cut, 0)

    spread_picks(z)
    count_rows(z)
    o = 1 - c
    cut_rows(0, c)
    arrived(0, table_piece(1, 0, c), tab_recv)
    ring(1, 0, 1, 4)
    cross(1, table_piece(1, 0, c))
    arrived(1, table_piece(3, 1, c), tab_recv)
    ring(3, 1, -1, 5)
    cross(2, table_piece(3, 1, c))
    def take_plane(d):
        came = lax.rem(z + 4 - d, 4)
        spread_picks(came)
        count_rows(came)

    def ids_from(d):
        return ids.at[pl.ds(lax.rem(z + 4 - d, 4) * 4, 4)]

    arrived(1, ids_from(1), ids_recv)
    take_plane(1)
    arrived(3, ids_from(3), ids_recv)
    take_plane(3)
    arrived(2, table_piece(1, 1, c), tab_recv)
    cross(1, table_piece(1, 1, c))
    arrived(3, table_piece(3, 0, c), tab_recv)
    cross(2, table_piece(3, 0, c))
    arrived(2, ids_from(2), ids_recv)
    take_plane(2)
    arrived(1, small.at[0, 0, pl.ds(0, 12)], small_recv)
    for d in (2, 1, 3):
        own = small.at[c, x]
        send(own, own, small_send.at[2], small_recv.at[2], peer(dx=d))
    arrived(0, table.at[x, o], core_recv)
    cut_rows(0, o)
    cut_rows(1, c)
    cut_rows(3, c)
    arrived(1, table.at[at_x(1), o], core_recv)
    arrived(2, table.at[at_x(3), o], core_recv)
    cut_rows(1, o)
    cut_rows(3, o)
    arrived(4, table_piece(2, 0, c), tab_recv)
    cross(3, table_piece(2, 0, c))
    arrived(5, table_piece(2, 1, c), tab_recv)
    cross(3, table_piece(2, 1, c))
    total[...] = jnp.dot(
        jnp.concatenate([count[at_x(s)].reshape(512, 1024) for s in (0, 1, 3)], axis=1),
        split[0:3].reshape(3072, 256),
        preferred_element_type=jnp.float32,
    ).reshape(4, 128, 256)
    cut_rows(2, c)
    arrived(3, table.at[at_x(2), o], core_recv)
    cut_rows(2, o)
    last = split[3].reshape(1024, 256)
    for dz in (2, 1, 3, 0):
        plane = lax.rem(z + dz, 4)
        new = total[plane] + jnp.dot(
            count[at_x(2), plane], last, preferred_element_type=jnp.float32
        )
        part[pl.ds(plane * 4, 4)] = (new[:, :128] + new[:, 128:]).reshape(4, 32, 128)
        for dy in (2, 1, 3, 0):
            if dz or dy:
                to = peer(dz=dz, dy=dy)
                send(
                    part.at[to[0] * 4 + to[1]], got.at[dz * 4 + dy],
                    sum_send.at[0], sum_recv.at[0], to,
                )
    arrived(2, small.at[0, pl.ds(0, 3)], small_recv)
    own = small.at[c]
    send(own, own, small_send.at[3], small_recv.at[3], peer(dc=1))
    arrived(3, small.at[o], small_recv)
    load_dense.wait()
    for load in load_ids:
        load.wait()

    def small_row(i):
        core, place = lax.rem(lax.div(i, 4), 2), lax.rem(lax.div(i, 8), 4)
        return small[core, place, lax.div(i, 32), pl.ds(lax.rem(i, 4), 1), :]

    for e in range(32):
        lhs_rows[e : e + 1, :] = small_row(small_ids[e])
        scale_rows[e : e + 1, :] = small_row(scale_ids[e])
    rows = lhs_rows[...]
    scaled = dense[...] * scale_rows[...]
    out_ref[2] = scaled * rows

    pooled = part[zy]
    arrived(0, got.at[pl.ds(1, 15)], sum_recv)
    for j in range(1, 16):
        pooled = pooled + got[j]
    pooled = pooled * PICKS ** (-0.5)
    out_ref[0] = scaled * pooled
    out_ref[1] = pooled * rows
    arrived(0, table.at[pl.ds(0, 3), 0], tab_send)
    arrived(0, table.at[:, 0], core_send)
    arrived(0, ids.at[pl.ds(0, 3)], ids_send)
    arrived(1, ids.at[pl.ds(0, 12)], ids_send)
    arrived(0, small.at[0, 0, pl.ds(0, 3)], small_send)
    arrived(1, small.at[0, 0, pl.ds(0, 12)], small_send)
    arrived(2, small.at[0, pl.ds(0, 3)], small_send)
    arrived(3, small.at[0], small_send)
    arrived(0, got.at[pl.ds(1, 15)], sum_send)


def on_device(picked_rows, main_table, dense_part, small_ids, small_table, scale_ids):
    dma = pltpu.SemaphoreType.DMA
    f32 = jnp.float32
    out = pl.pallas_call(
        kernel,
        out_shape=pltpu.VMEM((3, 32, 128), f32),
        in_specs=[pl.BlockSpec(memory_space=pl.ANY)] * 6,
        out_specs=pl.BlockSpec(memory_space=pltpu.VMEM),
        scratch_shapes=[
            pltpu.SMEM((32,), jnp.int32),
            pltpu.SMEM((32,), jnp.int32),
            pltpu.VMEM((8, 32), jnp.int32),
            pltpu.VMEM((16, 8, 32), jnp.int32),
            pltpu.VMEM((8, 4, 128, 256), jnp.int16),
            pltpu.VMEM((4, 4, 128, 1024), jnp.bfloat16),
            pltpu.VMEM((4, 2, 512, 128), f32),
            pltpu.VMEM((4, 2, 512, 256), jnp.bfloat16),
            pltpu.VMEM((4, 128, 256), f32),
            pltpu.VMEM((16, 32, 128), f32),
            pltpu.VMEM((16, 32, 128), f32),
            pltpu.VMEM((2, 4, 16, 4, 128), f32),
            pltpu.VMEM((32, 128), f32),
            pltpu.VMEM((32, 128), f32),
            pltpu.VMEM((32, 128), f32),
            dma((6,)), dma((2,)), dma((4,)), dma((1,)), dma((6,)), dma((1,)), dma((4,)),
            dma((4,)), dma((4,)), dma((1,)), dma((1,)),
        ],
        compiler_params=pltpu.CompilerParams(collective_id=0, has_side_effects=True),
    )(picked_rows.T, main_table, dense_part, small_table, small_ids, scale_ids)
    return out.transpose(1, 0, 2)


def solution(mesh):
    split = Mesh(mesh.devices.reshape(4, 4, 4, 2), SHARD)
    placed = (P(SHARD, None), P(SHARD, None), P(SHARD, None), P(SHARD), P(SHARD, None), P(SHARD))
    return jax.shard_map(
        on_device, mesh=split, in_specs=placed, out_specs=P(SHARD, None, None), check_vma=False
    )
```

```python
import functools

import jax
import jax.numpy as jnp
from jax import lax
from jax.experimental import pallas as pl
from jax.experimental.pallas import tpu as pltpu
from jax.sharding import Mesh
from jax.sharding import PartitionSpec as P

PICKS = 8
SHARD = ("z", "y", "x", "c")
MESH = pl.DeviceIdType.MESH


def kernel(
    picks_hbm, table_hbm, dense_hbm, small_hbm, small_ids_hbm, scale_ids_hbm,
    out_ref,
    small_ids, scale_ids, picks_in, ids, spread, count, table, split, total, part, got, small, dense, lhs_rows, scale_rows,
    load_sem, ids_send, ids_recv, tab_send, tab_recv, core_send, core_recv,
    small_send, small_recv, sum_send, sum_recv,
):
    z, y, x, c = (lax.axis_index(a) for a in SHARD)
    zy = z * 4 + y

    def peer(dz=0, dy=0, dx=0, dc=0):
        return (
            lax.rem(z + dz, 4), lax.rem(y + dy, 4), lax.rem(x + dx, 4), lax.rem(c + dc, 2)
        )

    def at_x(s):
        return lax.rem(x + 4 - s, 4)

    def send(src, dst, send_sem, recv_sem, to):
        copy = pltpu.make_async_remote_copy(
            src_ref=src, dst_ref=dst, send_sem=send_sem, recv_sem=recv_sem,
            device_id=to, device_id_type=MESH,
        )
        copy.start()
        return copy

    half = 256
    load_picks = pltpu.make_async_copy(picks_hbm, picks_in, load_sem.at[0])
    load_table = pltpu.make_async_copy(table_hbm, table.at[x, c], load_sem.at[1])
    load_small = pltpu.make_async_copy(small_hbm, small.at[c, x, zy], load_sem.at[2])
    load_dense = pltpu.make_async_copy(dense_hbm, dense, load_sem.at[3])
    load_table.start()
    load_picks.start()
    load_small.start()
    load_dense.start()
    load_ids = [
        pltpu.make_async_copy(small_ids_hbm, small_ids, load_sem.at[4]),
        pltpu.make_async_copy(scale_ids_hbm, scale_ids, load_sem.at[5]),
    ]
    for load in load_ids:
        load.start()

    axis_peers = (
        [peer(dx=d) for d in (1, 2, 3)] + [peer(dc=1)]
        + [peer(dy=d) for d in (1, 2, 3)] + [peer(dz=d) for d in (1, 2, 3)]
    )
    barrier = pltpu.get_barrier_semaphore()
    for who in axis_peers:
        pl.semaphore_signal(barrier, inc=1, device_id=who, device_id_type=MESH)
    pl.semaphore_wait(barrier, len(axis_peers))


    def table_piece(s, h, core):
        return table.at[at_x(s), core, pl.ds(h * half, half)]

    def ring(s, h, step, k):
        piece = table_piece(s, h, c)
        send(piece, piece, tab_send.at[0], tab_recv.at[k], peer(dx=step % 4))

    def arrived(k, piece, sem):
        pltpu.make_async_copy(piece, piece, sem.at[k]).wait()

    def cross(k, piece):
        send(piece, piece, core_send.at[0], core_recv.at[k], peer(dc=1))

    load_picks.wait()
    ids[zy] = picks_in[...]
    for d in (2, 1, 3):
        send(ids.at[zy], ids.at[zy], ids_send.at[0], ids_recv.at[0], peer(dy=d))
    load_table.wait()
    ring(0, 0, 1, 0)
    ring(0, 1, -1, 1)
    ring(0, 1, 1, 2)
    ring(0, 0, -1, 3)
    cross(0, table.at[x, c])
    load_small.wait()
    for d in (2, 1, 3):
        own = small.at[c, x, zy]
        send(own, own, small_send.at[0], small_recv.at[0], peer(dy=d))
    arrived(0, ids.at[pl.ds(0, 3)], ids_recv)
    mine = pl.ds(z * 4, 4)
    for d in (2, 1, 3):
        send(ids.at[mine], ids.at[mine], ids_send.at[1], ids_recv.at[d], peer(dz=d))
    arrived(0, small.at[0, 0, pl.ds(0, 3)], small_recv)
    for d in (1, 2, 3):
        own = small.at[c, x, mine]
        send(own, own, small_send.at[1], small_recv.at[1], peer(dz=d))

    first = zy * 4096

    def spread_picks(plane):
        for b in range(4):
            block = jnp.clip(ids[plane * 4 + b] - first, -1, 4096)
            block = jnp.concatenate([block, jnp.zeros((8, 96), jnp.int32)], axis=1)
            columns = jnp.transpose(block)[:32]
            for k in range(PICKS):
                spread[k, plane, b * 32 : (b + 1) * 32, :] = jnp.broadcast_to(
                    columns[:, k : k + 1], (32, 256)
                ).astype(jnp.int16)

    one, none = jnp.ones((16, 256), jnp.bfloat16), jnp.zeros((16, 256), jnp.bfloat16)
    lane = lax.broadcasted_iota(jnp.int32, (16, 256), 1).astype(jnp.int16)

    def count_rows(plane):
        def tile(t, carry):
            at = pl.ds(pl.multiple_of(t * 16, 16), 16)
            wanted = [spread[k, plane, at, :] for k in range(PICKS)]
            for place in range(4):
                for q in range(4):
                    here = lane + jnp.int16(place * 1024 + q * 256)
                    hits = [jnp.where(w == here, one, none) for w in wanted]
                    while len(hits) > 1:
                        hits = [a + b for a, b in zip(hits[::2], hits[1::2])]
                    count[place, q // 2, plane, at, q % 2 * 256 : (q % 2 + 1) * 256] = hits[0]
            return carry

        lax.fori_loop(0, 8, tile, 0)

    def cut_rows(s, core):
        def cut(t, carry):
            at = pl.ds(pl.multiple_of(t * 128, 128), 128)
            rows = table[at_x(s), core, at]
            high = rows.astype(jnp.bfloat16)
            low = (rows - high.astype(jnp.float32)).astype(jnp.bfloat16)
            split[(0, 1, 3, 2)[s], core, at, 0:128] = high
            split[(0, 1, 3, 2)[s], core, at, 128:256] = low
            return carry

        lax.fori_loop(0, 4, cut, 0)

    spread_picks(z)
    count_rows(z)
    o = 1 - c
    cut_rows(0, c)
    arrived(0, table_piece(1, 0, c), tab_recv)
    ring(1, 0, 1, 4)
    cross(1, table_piece(1, 0, c))
    arrived(1, table_piece(3, 1, c), tab_recv)
    ring(3, 1, -1, 5)
    cross(2, table_piece(3, 1, c))
    def take_plane(d):
        came = lax.rem(z + 4 - d, 4)
        spread_picks(came)
        count_rows(came)

    def ids_from(d):
        return ids.at[pl.ds(lax.rem(z + 4 - d, 4) * 4, 4)]

    arrived(3, ids_from(3), ids_recv)
    take_plane(3)
    arrived(1, ids_from(1), ids_recv)
    take_plane(1)
    arrived(2, table_piece(1, 1, c), tab_recv)
    cross(1, table_piece(1, 1, c))
    arrived(3, table_piece(3, 0, c), tab_recv)
    cross(2, table_piece(3, 0, c))
    arrived(2, ids_from(2), ids_recv)
    take_plane(2)
    arrived(1, small.at[0, 0, pl.ds(0, 12)], small_recv)
    for d in (2, 1, 3):
        own = small.at[c, x]
        send(own, own, small_send.at[2], small_recv.at[2], peer(dx=d))
    arrived(0, table.at[x, o], core_recv)
    cut_rows(0, o)
    cut_rows(1, c)
    cut_rows(3, c)
    def product(pieces):
        lhs = [count[at_x(s), core].reshape(512, 512) for s, core in pieces]
        rhs = [split[(0, 1, 3, 2)[s], core] for s, core in pieces]
        return jnp.dot(
            jnp.concatenate(lhs, axis=1), jnp.concatenate(rhs, axis=0),
            preferred_element_type=jnp.float32,
        ).reshape(4, 128, 256)

    arrived(4, table_piece(2, 0, c), tab_recv)
    cross(3, table_piece(2, 0, c))
    arrived(5, table_piece(2, 1, c), tab_recv)
    cross(3, table_piece(2, 1, c))
    total[...] = product(((0, c), (0, o), (1, c), (3, c)))
    arrived(1, table.at[at_x(1), o], core_recv)
    arrived(2, table.at[at_x(3), o], core_recv)
    cut_rows(1, o)
    cut_rows(3, o)
    cut_rows(2, c)
    total[...] = total[...] + product(((1, o), (3, o), (2, c)))
    arrived(3, table.at[at_x(2), o], core_recv)
    cut_rows(2, o)
    last = split[3, o]
    for dz in (2, 1, 3, 0):
        plane = lax.rem(z + dz, 4)
        new = total[plane] + jnp.dot(
            count[at_x(2), o, plane], last, preferred_element_type=jnp.float32
        )
        part[pl.ds(plane * 4, 4)] = (new[:, :128] + new[:, 128:]).reshape(4, 32, 128)
        for dy in (2, 1, 3, 0):
            if dz or dy:
                to = peer(dz=dz, dy=dy)
                send(
                    part.at[to[0] * 4 + to[1]], got.at[dz * 4 + dy],
                    sum_send.at[0], sum_recv.at[0], to,
                )
    arrived(2, small.at[0, pl.ds(0, 3)], small_recv)
    own = small.at[c]
    send(own, own, small_send.at[3], small_recv.at[3], peer(dc=1))
    arrived(3, small.at[o], small_recv)
    load_dense.wait()
    for load in load_ids:
        load.wait()

    def small_row(i):
        core, place = lax.rem(lax.div(i, 4), 2), lax.rem(lax.div(i, 8), 4)
        return small[core, place, lax.div(i, 32), pl.ds(lax.rem(i, 4), 1), :]

    for e in range(32):
        lhs_rows[e : e + 1, :] = small_row(small_ids[e])
        scale_rows[e : e + 1, :] = small_row(scale_ids[e])
    rows = lhs_rows[...]
    scaled = dense[...] * scale_rows[...]
    out_ref[2] = scaled * rows

    pooled = part[zy]
    arrived(0, got.at[pl.ds(1, 15)], sum_recv)
    for j in range(1, 16):
        pooled = pooled + got[j]
    pooled = pooled * PICKS ** (-0.5)
    out_ref[0] = scaled * pooled
    out_ref[1] = pooled * rows
    arrived(0, table.at[pl.ds(0, 3), 0], tab_send)
    arrived(0, table.at[:, 0], core_send)
    arrived(0, ids.at[pl.ds(0, 3)], ids_send)
    arrived(1, ids.at[pl.ds(0, 12)], ids_send)
    arrived(0, small.at[0, 0, pl.ds(0, 3)], small_send)
    arrived(1, small.at[0, 0, pl.ds(0, 12)], small_send)
    arrived(2, small.at[0, pl.ds(0, 3)], small_send)
    arrived(3, small.at[0], small_send)
    arrived(0, got.at[pl.ds(1, 15)], sum_send)


def on_device(picked_rows, main_table, dense_part, small_ids, small_table, scale_ids):
    dma = pltpu.SemaphoreType.DMA
    f32 = jnp.float32
    out = pl.pallas_call(
        kernel,
        out_shape=pltpu.VMEM((3, 32, 128), f32),
        in_specs=[pl.BlockSpec(memory_space=pl.ANY)] * 6,
        out_specs=pl.BlockSpec(memory_space=pltpu.VMEM),
        scratch_shapes=[
            pltpu.SMEM((32,), jnp.int32),
            pltpu.SMEM((32,), jnp.int32),
            pltpu.VMEM((8, 32), jnp.int32),
            pltpu.VMEM((16, 8, 32), jnp.int32),
            pltpu.VMEM((8, 4, 128, 256), jnp.int16),
            pltpu.VMEM((4, 2, 4, 128, 512), jnp.bfloat16),
            pltpu.VMEM((4, 2, 512, 128), f32),
            pltpu.VMEM((4, 2, 512, 256), jnp.bfloat16),
            pltpu.VMEM((4, 128, 256), f32),
            pltpu.VMEM((16, 32, 128), f32),
            pltpu.VMEM((16, 32, 128), f32),
            pltpu.VMEM((2, 4, 16, 4, 128), f32),
            pltpu.VMEM((32, 128), f32),
            pltpu.VMEM((32, 128), f32),
            pltpu.VMEM((32, 128), f32),
            dma((6,)), dma((2,)), dma((4,)), dma((1,)), dma((6,)), dma((1,)), dma((4,)),
            dma((4,)), dma((4,)), dma((1,)), dma((1,)),
        ],
        compiler_params=pltpu.CompilerParams(collective_id=0, has_side_effects=True),
    )(picked_rows.T, main_table, dense_part, small_table, small_ids, scale_ids)
    return out.transpose(1, 0, 2)


def solution(mesh):
    split = Mesh(mesh.devices.reshape(4, 4, 4, 2), SHARD)
    placed = (P(SHARD, None), P(SHARD, None), P(SHARD, None), P(SHARD), P(SHARD, None), P(SHARD))
    return jax.shard_map(
        on_device, mesh=split, in_specs=placed, out_specs=P(SHARD, None, None), check_vma=False
    )
```

```python
import functools

import jax
import jax.numpy as jnp
from jax import lax
from jax.experimental import pallas as pl
from jax.experimental.pallas import tpu as pltpu
from jax.sharding import Mesh
from jax.sharding import PartitionSpec as P

PICKS = 8
SHARD = ("z", "y", "x", "c")
MESH = pl.DeviceIdType.MESH


def kernel(
    picks_hbm, table_hbm, dense_hbm, small_hbm, small_ids_hbm, scale_ids_hbm,
    out_ref,
    small_ids, scale_ids, picks_in, ids, spread, count, table, split, total, part, got, small, dense, lhs_rows, scale_rows,
    load_sem, ids_send, ids_recv, tab_send, tab_recv, core_send, core_recv,
    small_send, small_recv, sum_send, sum_recv,
):
    z, y, x, c = (lax.axis_index(a) for a in SHARD)
    zy = z * 4 + y

    def peer(dz=0, dy=0, dx=0, dc=0):
        return (
            lax.rem(z + dz, 4), lax.rem(y + dy, 4), lax.rem(x + dx, 4), lax.rem(c + dc, 2)
        )

    def at_x(s):
        return lax.rem(x + 4 - s, 4)

    def send(src, dst, send_sem, recv_sem, to):
        copy = pltpu.make_async_remote_copy(
            src_ref=src, dst_ref=dst, send_sem=send_sem, recv_sem=recv_sem,
            device_id=to, device_id_type=MESH,
        )
        copy.start()
        return copy

    half = 256
    load_picks = pltpu.make_async_copy(picks_hbm, picks_in, load_sem.at[0])
    load_table = pltpu.make_async_copy(table_hbm, table.at[x, c], load_sem.at[1])
    load_small = pltpu.make_async_copy(small_hbm, small.at[c, x, zy], load_sem.at[2])
    load_dense = pltpu.make_async_copy(dense_hbm, dense, load_sem.at[3])
    load_table.start()
    load_picks.start()
    load_small.start()
    load_dense.start()
    load_ids = [
        pltpu.make_async_copy(small_ids_hbm, small_ids, load_sem.at[4]),
        pltpu.make_async_copy(scale_ids_hbm, scale_ids, load_sem.at[5]),
    ]
    for load in load_ids:
        load.start()

    axis_peers = (
        [peer(dz=d) for d in (2, 1, 3)] + [peer(dy=d) for d in (2, 1, 3)]
        + [peer(dx=d) for d in (2, 1, 3)] + [peer(dc=1)]
    )
    barrier = pltpu.get_barrier_semaphore()
    for who in axis_peers:
        pl.semaphore_signal(barrier, inc=1, device_id=who, device_id_type=MESH)
    pl.semaphore_wait(barrier, len(axis_peers))


    def table_piece(s, h, core):
        return table.at[at_x(s), core, pl.ds(h * half, half)]

    def ring(s, h, step, k):
        piece = table_piece(s, h, c)
        send(piece, piece, tab_send.at[0], tab_recv.at[k], peer(dx=step % 4))

    def arrived(k, piece, sem):
        pltpu.make_async_copy(piece, piece, sem.at[k]).wait()

    def cross(k, piece):
        send(piece, piece, core_send.at[0], core_recv.at[k], peer(dc=1))

    load_picks.wait()
    ids[zy] = picks_in[...]
    for d in (2, 1, 3):
        send(ids.at[zy], ids.at[zy], ids_send.at[0], ids_recv.at[0], peer(dy=d))
    load_table.wait()
    ring(0, 0, 1, 0)
    ring(0, 1, -1, 1)
    ring(0, 1, 1, 2)
    ring(0, 0, -1, 3)
    cross(0, table.at[x, c])
    load_small.wait()
    for d in (2, 1, 3):
        own = small.at[c, x, zy]
        send(own, own, small_send.at[0], small_recv.at[0], peer(dy=d))
    arrived(0, ids.at[pl.ds(0, 3)], ids_recv)
    mine = pl.ds(z * 4, 4)
    for d in (2, 1, 3):
        send(ids.at[mine], ids.at[mine], ids_send.at[1], ids_recv.at[d], peer(dz=d))
    arrived(0, small.at[0, 0, pl.ds(0, 3)], small_recv)
    for d in (1, 2, 3):
        own = small.at[c, x, mine]
        send(own, own, small_send.at[1], small_recv.at[1], peer(dz=d))

    first = zy * 4096

    def spread_picks(plane):
        for b in range(4):
            block = jnp.clip(ids[plane * 4 + b] - first, -1, 4096)
            block = jnp.concatenate([block, jnp.zeros((8, 96), jnp.int32)], axis=1)
            columns = jnp.transpose(block)[:32]
            for k in range(PICKS):
                spread[k, plane, b * 32 : (b + 1) * 32, :] = jnp.broadcast_to(
                    columns[:, k : k + 1], (32, 256)
                ).astype(jnp.int16)

    one, none = jnp.ones((16, 256), jnp.bfloat16), jnp.zeros((16, 256), jnp.bfloat16)
    lane = lax.broadcasted_iota(jnp.int32, (16, 256), 1).astype(jnp.int16)

    def count_rows(plane):
        def tile(t, carry):
            at = pl.ds(pl.multiple_of(t * 16, 16), 16)
            wanted = [spread[k, plane, at, :] for k in range(PICKS)]
            for place in range(4):
                for q in range(4):
                    here = lane + jnp.int16(place * 1024 + q * 256)
                    hits = [jnp.where(w == here, one, none) for w in wanted]
                    while len(hits) > 1:
                        hits = [a + b for a, b in zip(hits[::2], hits[1::2])]
                    count[place, q // 2, plane, at, q % 2 * 256 : (q % 2 + 1) * 256] = hits[0]
            return carry

        lax.fori_loop(0, 8, tile, 0)

    def cut_rows(s, core):
        def cut(t, carry):
            at = pl.ds(pl.multiple_of(t * 128, 128), 128)
            rows = table[at_x(s), core, at]
            high = rows.astype(jnp.bfloat16)
            low = (rows - high.astype(jnp.float32)).astype(jnp.bfloat16)
            split[(0, 1, 3, 2)[s], core, at, 0:128] = high
            split[(0, 1, 3, 2)[s], core, at, 128:256] = low
            return carry

        lax.fori_loop(0, 4, cut, 0)

    spread_picks(z)
    count_rows(z)
    o = 1 - c
    cut_rows(0, c)
    arrived(0, table_piece(1, 0, c), tab_recv)
    ring(1, 0, 1, 4)
    cross(1, table_piece(1, 0, c))
    arrived(1, table_piece(3, 1, c), tab_recv)
    ring(3, 1, -1, 5)
    cross(2, table_piece(3, 1, c))
    def take_plane(d):
        came = lax.rem(z + 4 - d, 4)
        spread_picks(came)
        count_rows(came)

    def ids_from(d):
        return ids.at[pl.ds(lax.rem(z + 4 - d, 4) * 4, 4)]

    arrived(3, ids_from(3), ids_recv)
    take_plane(3)
    arrived(1, ids_from(1), ids_recv)
    take_plane(1)
    arrived(2, table_piece(1, 1, c), tab_recv)
    cross(1, table_piece(1, 1, c))
    arrived(3, table_piece(3, 0, c), tab_recv)
    cross(2, table_piece(3, 0, c))
    arrived(2, ids_from(2), ids_recv)
    take_plane(2)
    arrived(1, small.at[0, 0, pl.ds(0, 12)], small_recv)
    for d in (2, 1, 3):
        own = small.at[c, x]
        send(own, own, small_send.at[2], small_recv.at[2], peer(dx=d))
    arrived(0, table.at[x, o], core_recv)
    cut_rows(0, o)
    cut_rows(1, c)
    cut_rows(3, c)
    def product(pieces):
        lhs = [count[at_x(s), core].reshape(512, 512) for s, core in pieces]
        rhs = [split[(0, 1, 3, 2)[s], core] for s, core in pieces]
        return jnp.dot(
            jnp.concatenate(lhs, axis=1), jnp.concatenate(rhs, axis=0),
            preferred_element_type=jnp.float32,
        ).reshape(4, 128, 256)

    arrived(4, table_piece(2, 0, c), tab_recv)
    cross(3, table_piece(2, 0, c))
    arrived(5, table_piece(2, 1, c), tab_recv)
    cross(3, table_piece(2, 1, c))
    total[...] = product(((0, c), (0, o), (1, c), (3, c)))
    arrived(1, table.at[at_x(1), o], core_recv)
    arrived(2, table.at[at_x(3), o], core_recv)
    cut_rows(1, o)
    cut_rows(3, o)
    cut_rows(2, c)
    total[...] = total[...] + product(((1, o), (3, o), (2, c)))
    arrived(3, table.at[at_x(2), o], core_recv)
    cut_rows(2, o)
    last = split[3, o]
    for pair in ((2, 1), (3, 0)):
        planes = [lax.rem(z + dz, 4) for dz in pair]
        lhs = jnp.concatenate([count[at_x(2), o, plane] for plane in planes], axis=0)
        new = jnp.dot(lhs, last, preferred_element_type=jnp.float32)
        for n, (dz, plane) in enumerate(zip(pair, planes)):
            here = total[plane] + new[n * 128 : (n + 1) * 128]
            part[pl.ds(plane * 4, 4)] = (here[:, :128] + here[:, 128:]).reshape(4, 32, 128)
            for dy in (2, 1, 3, 0):
                if dz or dy:
                    to = peer(dz=dz, dy=dy)
                    send(
                        part.at[to[0] * 4 + to[1]], got.at[dz * 4 + dy],
                        sum_send.at[0], sum_recv.at[0], to,
                    )
    arrived(2, small.at[0, pl.ds(0, 3)], small_recv)
    own = small.at[c]
    send(own, own, small_send.at[3], small_recv.at[3], peer(dc=1))
    arrived(3, small.at[o], small_recv)
    load_dense.wait()
    for load in load_ids:
        load.wait()

    def small_row(i):
        core, place = lax.rem(lax.div(i, 4), 2), lax.rem(lax.div(i, 8), 4)
        return small[core, place, lax.div(i, 32), pl.ds(lax.rem(i, 4), 1), :]

    for e in range(32):
        lhs_rows[e : e + 1, :] = small_row(small_ids[e])
        scale_rows[e : e + 1, :] = small_row(scale_ids[e])
    rows = lhs_rows[...]
    scaled = dense[...] * scale_rows[...]
    out_ref[2] = scaled * rows

    pooled = part[zy]
    arrived(0, got.at[pl.ds(1, 15)], sum_recv)
    for j in range(1, 16):
        pooled = pooled + got[j]
    pooled = pooled * PICKS ** (-0.5)
    out_ref[0] = scaled * pooled
    out_ref[1] = pooled * rows
    arrived(0, table.at[pl.ds(0, 3), 0], tab_send)
    arrived(0, table.at[:, 0], core_send)
    arrived(0, ids.at[pl.ds(0, 3)], ids_send)
    arrived(1, ids.at[pl.ds(0, 12)], ids_send)
    arrived(0, small.at[0, 0, pl.ds(0, 3)], small_send)
    arrived(1, small.at[0, 0, pl.ds(0, 12)], small_send)
    arrived(2, small.at[0, pl.ds(0, 3)], small_send)
    arrived(3, small.at[0], small_send)
    arrived(0, got.at[pl.ds(1, 15)], sum_send)


def on_device(picked_rows, main_table, dense_part, small_ids, small_table, scale_ids):
    dma = pltpu.SemaphoreType.DMA
    f32 = jnp.float32
    out = pl.pallas_call(
        kernel,
        out_shape=pltpu.VMEM((3, 32, 128), f32),
        in_specs=[pl.BlockSpec(memory_space=pl.ANY)] * 6,
        out_specs=pl.BlockSpec(memory_space=pltpu.VMEM),
        scratch_shapes=[
            pltpu.SMEM((32,), jnp.int32),
            pltpu.SMEM((32,), jnp.int32),
            pltpu.VMEM((8, 32), jnp.int32),
            pltpu.VMEM((16, 8, 32), jnp.int32),
            pltpu.VMEM((8, 4, 128, 256), jnp.int16),
            pltpu.VMEM((4, 2, 4, 128, 512), jnp.bfloat16),
            pltpu.VMEM((4, 2, 512, 128), f32),
            pltpu.VMEM((4, 2, 512, 256), jnp.bfloat16),
            pltpu.VMEM((4, 128, 256), f32),
            pltpu.VMEM((16, 32, 128), f32),
            pltpu.VMEM((16, 32, 128), f32),
            pltpu.VMEM((2, 4, 16, 4, 128), f32),
            pltpu.VMEM((32, 128), f32),
            pltpu.VMEM((32, 128), f32),
            pltpu.VMEM((32, 128), f32),
            dma((6,)), dma((2,)), dma((4,)), dma((1,)), dma((6,)), dma((1,)), dma((4,)),
            dma((4,)), dma((4,)), dma((1,)), dma((1,)),
        ],
        compiler_params=pltpu.CompilerParams(collective_id=0, has_side_effects=True),
    )(picked_rows.T, main_table, dense_part, small_table, small_ids, scale_ids)
    return out.transpose(1, 0, 2)


def solution(mesh):
    split = Mesh(mesh.devices.reshape(4, 4, 4, 2), SHARD)
    placed = (P(SHARD, None), P(SHARD, None), P(SHARD, None), P(SHARD), P(SHARD, None), P(SHARD))
    return jax.shard_map(
        on_device, mesh=split, in_specs=placed, out_specs=P(SHARD, None, None), check_vma=False
    )
```

```python
import functools

import jax
import jax.numpy as jnp
from jax import lax
from jax.experimental import pallas as pl
from jax.experimental.pallas import tpu as pltpu
from jax.sharding import Mesh
from jax.sharding import PartitionSpec as P

PICKS = 8
SHARD = ("z", "y", "x", "c")
MESH = pl.DeviceIdType.MESH


def kernel(
    picks_hbm, table_hbm, dense_hbm, small_hbm, small_ids_hbm, scale_ids_hbm,
    out_ref,
    small_ids, scale_ids, picks_in, ids, spread, count, table, split, total, part, got, small, dense, lhs_rows, scale_rows,
    load_sem, ids_send, ids_recv, tab_send, tab_recv, core_send, core_recv,
    small_send, small_recv, sum_send, sum_recv,
):
    z, y, x, c = (lax.axis_index(a) for a in SHARD)
    zy = z * 4 + y

    def peer(dz=0, dy=0, dx=0, dc=0):
        return (
            lax.rem(z + dz, 4), lax.rem(y + dy, 4), lax.rem(x + dx, 4), lax.rem(c + dc, 2)
        )

    def at_x(s):
        return lax.rem(x + 4 - s, 4)

    def send(src, dst, send_sem, recv_sem, to):
        copy = pltpu.make_async_remote_copy(
            src_ref=src, dst_ref=dst, send_sem=send_sem, recv_sem=recv_sem,
            device_id=to, device_id_type=MESH,
        )
        copy.start()
        return copy

    half = 256
    load_picks = pltpu.make_async_copy(picks_hbm, picks_in, load_sem.at[0])
    load_table = pltpu.make_async_copy(table_hbm, table.at[x, c], load_sem.at[1])
    load_small = pltpu.make_async_copy(small_hbm, small.at[c, x, zy], load_sem.at[2])
    load_dense = pltpu.make_async_copy(dense_hbm, dense, load_sem.at[3])
    load_table.start()
    load_picks.start()
    load_small.start()
    load_dense.start()
    load_ids = [
        pltpu.make_async_copy(small_ids_hbm, small_ids, load_sem.at[4]),
        pltpu.make_async_copy(scale_ids_hbm, scale_ids, load_sem.at[5]),
    ]
    for load in load_ids:
        load.start()

    axis_peers = (
        [peer(dz=d) for d in (2, 1, 3)] + [peer(dy=d) for d in (2, 1, 3)]
        + [peer(dx=d) for d in (2, 1, 3)] + [peer(dc=1)]
    )
    barrier = pltpu.get_barrier_semaphore()
    for who in axis_peers:
        pl.semaphore_signal(barrier, inc=1, device_id=who, device_id_type=MESH)
    pl.semaphore_wait(barrier, len(axis_peers))


    def table_piece(s, h, core):
        return table.at[at_x(s), core, pl.ds(h * half, half)]

    def ring(s, h, step, k):
        piece = table_piece(s, h, c)
        send(piece, piece, tab_send.at[0], tab_recv.at[k], peer(dx=step % 4))

    def arrived(k, piece, sem):
        pltpu.make_async_copy(piece, piece, sem.at[k]).wait()

    def cross(k, piece):
        send(piece, piece, core_send.at[0], core_recv.at[k], peer(dc=1))

    load_picks.wait()
    ids[zy] = picks_in[...]
    for d in (2, 1, 3):
        send(ids.at[zy], ids.at[zy], ids_send.at[0], ids_recv.at[0], peer(dy=d))
    load_table.wait()
    ring(0, 0, 1, 0)
    ring(0, 1, -1, 1)
    ring(0, 1, 1, 2)
    ring(0, 0, -1, 3)
    cross(0, table.at[x, c])
    load_small.wait()
    for d in (2, 1, 3):
        own = small.at[c, x, zy]
        send(own, own, small_send.at[0], small_recv.at[0], peer(dy=d))
    arrived(0, ids.at[pl.ds(0, 3)], ids_recv)
    mine = pl.ds(z * 4, 4)
    for d in (2, 1, 3):
        send(ids.at[mine], ids.at[mine], ids_send.at[1], ids_recv.at[d], peer(dz=d))
    arrived(0, small.at[0, 0, pl.ds(0, 3)], small_recv)
    for d in (1, 2, 3):
        own = small.at[c, x, mine]
        send(own, own, small_send.at[1], small_recv.at[1], peer(dz=d))

    first = zy * 4096

    def spread_picks(plane):
        for b in range(4):
            block = jnp.clip(ids[plane * 4 + b] - first, -1, 4096)
            block = jnp.concatenate([block, jnp.zeros((8, 96), jnp.int32)], axis=1)
            columns = jnp.transpose(block)[:32]
            for k in range(PICKS):
                spread[k, plane, b * 32 : (b + 1) * 32, :] = jnp.broadcast_to(
                    columns[:, k : k + 1], (32, 256)
                ).astype(jnp.int16)

    one, none = jnp.ones((16, 256), jnp.bfloat16), jnp.zeros((16, 256), jnp.bfloat16)
    lane = lax.broadcasted_iota(jnp.int32, (16, 256), 1).astype(jnp.int16)

    def count_rows(plane):
        def tile(t, carry):
            at = pl.ds(pl.multiple_of(t * 16, 16), 16)
            wanted = [spread[k, plane, at, :] for k in range(PICKS)]
            for place in range(4):
                for q in range(4):
                    here = lane + jnp.int16(place * 1024 + q * 256)
                    hits = [jnp.where(w == here, one, none) for w in wanted]
                    while len(hits) > 1:
                        hits = [a + b for a, b in zip(hits[::2], hits[1::2])]
                    count[place, q // 2, plane, at, q % 2 * 256 : (q % 2 + 1) * 256] = hits[0]
            return carry

        lax.fori_loop(0, 8, tile, 0)

    def cut_rows(s, core):
        def cut(t, carry):
            at = pl.ds(pl.multiple_of(t * 128, 128), 128)
            rows = table[at_x(s), core, at]
            high = rows.astype(jnp.bfloat16)
            low = (rows - high.astype(jnp.float32)).astype(jnp.bfloat16)
            split[(0, 1, 3, 2)[s], core, at, 0:128] = high
            split[(0, 1, 3, 2)[s], core, at, 128:256] = low
            return carry

        lax.fori_loop(0, 4, cut, 0)

    spread_picks(z)
    count_rows(z)
    o = 1 - c
    cut_rows(0, c)
    arrived(0, table_piece(1, 0, c), tab_recv)
    ring(1, 0, 1, 4)
    cross(1, table_piece(1, 0, c))
    arrived(1, table_piece(3, 1, c), tab_recv)
    ring(3, 1, -1, 5)
    cross(2, table_piece(3, 1, c))
    def take_plane(d):
        came = lax.rem(z + 4 - d, 4)
        spread_picks(came)
        count_rows(came)

    def ids_from(d):
        return ids.at[pl.ds(lax.rem(z + 4 - d, 4) * 4, 4)]

    arrived(3, ids_from(3), ids_recv)
    take_plane(3)
    arrived(1, ids_from(1), ids_recv)
    take_plane(1)
    arrived(2, table_piece(1, 1, c), tab_recv)
    cross(1, table_piece(1, 1, c))
    arrived(3, table_piece(3, 0, c), tab_recv)
    cross(2, table_piece(3, 0, c))
    arrived(2, ids_from(2), ids_recv)
    take_plane(2)
    arrived(1, small.at[0, 0, pl.ds(0, 12)], small_recv)
    for d in (2, 1, 3):
        own = small.at[c, x]
        send(own, own, small_send.at[2], small_recv.at[2], peer(dx=d))
    arrived(0, table.at[x, o], core_recv)
    cut_rows(0, o)
    arrived(4, table_piece(2, 0, c), tab_recv)
    cross(3, table_piece(2, 0, c))
    arrived(5, table_piece(2, 1, c), tab_recv)
    cross(3, table_piece(2, 1, c))
    cut_rows(1, c)
    cut_rows(3, c)
    def product(pieces):
        lhs = [count[at_x(s), core].reshape(512, 512) for s, core in pieces]
        rhs = [split[(0, 1, 3, 2)[s], core] for s, core in pieces]
        return jnp.dot(
            jnp.concatenate(lhs, axis=1), jnp.concatenate(rhs, axis=0),
            preferred_element_type=jnp.float32,
        ).reshape(4, 128, 256)

    total[...] = product(((0, c), (0, o), (1, c), (3, c)))
    arrived(1, table.at[at_x(1), o], core_recv)
    arrived(2, table.at[at_x(3), o], core_recv)
    cut_rows(1, o)
    cut_rows(3, o)
    cut_rows(2, c)
    total[...] = total[...] + product(((1, o), (3, o), (2, c)))
    arrived(3, table.at[at_x(2), o], core_recv)
    cut_rows(2, o)
    last = split[3, o]
    for pair in ((2, 1), (3, 0)):
        planes = [lax.rem(z + dz, 4) for dz in pair]
        lhs = jnp.concatenate([count[at_x(2), o, plane] for plane in planes], axis=0)
        new = jnp.dot(lhs, last, preferred_element_type=jnp.float32)
        for n, (dz, plane) in enumerate(zip(pair, planes)):
            here = total[plane] + new[n * 128 : (n + 1) * 128]
            part[pl.ds(plane * 4, 4)] = (here[:, :128] + here[:, 128:]).reshape(4, 32, 128)
            for dy in (2, 1, 3, 0):
                if dz or dy:
                    to = peer(dz=dz, dy=dy)
                    send(
                        part.at[to[0] * 4 + to[1]], got.at[dz * 4 + dy],
                        sum_send.at[0], sum_recv.at[0], to,
                    )
    arrived(2, small.at[0, pl.ds(0, 3)], small_recv)
    own = small.at[c]
    send(own, own, small_send.at[3], small_recv.at[3], peer(dc=1))
    arrived(3, small.at[o], small_recv)
    load_dense.wait()
    for load in load_ids:
        load.wait()

    def small_row(i):
        core, place = lax.rem(lax.div(i, 4), 2), lax.rem(lax.div(i, 8), 4)
        return small[core, place, lax.div(i, 32), pl.ds(lax.rem(i, 4), 1), :]

    for e in range(32):
        lhs_rows[e : e + 1, :] = small_row(small_ids[e])
        scale_rows[e : e + 1, :] = small_row(scale_ids[e])
    rows = lhs_rows[...]
    scaled = dense[...] * scale_rows[...]
    out_ref[2] = scaled * rows

    pooled = part[zy]
    arrived(0, got.at[pl.ds(1, 15)], sum_recv)
    for j in range(1, 16):
        pooled = pooled + got[j]
    pooled = pooled * PICKS ** (-0.5)
    out_ref[0] = scaled * pooled
    out_ref[1] = pooled * rows
    arrived(0, table.at[pl.ds(0, 3), 0], tab_send)
    arrived(0, table.at[:, 0], core_send)
    arrived(0, ids.at[pl.ds(0, 3)], ids_send)
    arrived(1, ids.at[pl.ds(0, 12)], ids_send)
    arrived(0, small.at[0, 0, pl.ds(0, 3)], small_send)
    arrived(1, small.at[0, 0, pl.ds(0, 12)], small_send)
    arrived(2, small.at[0, pl.ds(0, 3)], small_send)
    arrived(3, small.at[0], small_send)
    arrived(0, got.at[pl.ds(1, 15)], sum_send)


def on_device(picked_rows, main_table, dense_part, small_ids, small_table, scale_ids):
    dma = pltpu.SemaphoreType.DMA
    f32 = jnp.float32
    out = pl.pallas_call(
        kernel,
        out_shape=pltpu.VMEM((3, 32, 128), f32),
        in_specs=[pl.BlockSpec(memory_space=pl.ANY)] * 6,
        out_specs=pl.BlockSpec(memory_space=pltpu.VMEM),
        scratch_shapes=[
            pltpu.SMEM((32,), jnp.int32),
            pltpu.SMEM((32,), jnp.int32),
            pltpu.VMEM((8, 32), jnp.int32),
            pltpu.VMEM((16, 8, 32), jnp.int32),
            pltpu.VMEM((8, 4, 128, 256), jnp.int16),
            pltpu.VMEM((4, 2, 4, 128, 512), jnp.bfloat16),
            pltpu.VMEM((4, 2, 512, 128), f32),
            pltpu.VMEM((4, 2, 512, 256), jnp.bfloat16),
            pltpu.VMEM((4, 128, 256), f32),
            pltpu.VMEM((16, 32, 128), f32),
            pltpu.VMEM((16, 32, 128), f32),
            pltpu.VMEM((2, 4, 16, 4, 128), f32),
            pltpu.VMEM((32, 128), f32),
            pltpu.VMEM((32, 128), f32),
            pltpu.VMEM((32, 128), f32),
            dma((6,)), dma((2,)), dma((4,)), dma((1,)), dma((6,)), dma((1,)), dma((4,)),
            dma((4,)), dma((4,)), dma((1,)), dma((1,)),
        ],
        compiler_params=pltpu.CompilerParams(collective_id=0, has_side_effects=True),
    )(picked_rows.T, main_table, dense_part, small_table, small_ids, scale_ids)
    return out.transpose(1, 0, 2)


def solution(mesh):
    split = Mesh(mesh.devices.reshape(4, 4, 4, 2), SHARD)
    placed = (P(SHARD, None), P(SHARD, None), P(SHARD, None), P(SHARD), P(SHARD, None), P(SHARD))
    return jax.shard_map(
        on_device, mesh=split, in_specs=placed, out_specs=P(SHARD, None, None), check_vma=False
    )
```
